256 devices in a mesh: groups: 4 (over y, x), blk: 32 (over z), span: 2 (over core).
Axes of the slice: x: 2, y: 2, z: 32, core: 2. Of those that a mesh axis runs over, the one named last changes fastest.
The devices are a block of a 4x8x32 slice.
Arguments:
- embeddings: bfloat16 [65536, 768], P(('groups', 'blk', 'span')), parts along dimension 0, may hold values from -6 to 6
- owner_ids: int32 [65536, 1], P(('groups', 'blk', 'span')), parts along dimension 0, may hold values from 0 to 31, as said below
- local_ids: int32 [65536], P(('groups', 'blk', 'span')), parts along dimension 0, may hold values from 0 to 15, as said below
- cluster_map: int32 [2048], P('groups'), parts along dimension 0, may hold values from 0 to 511, as said below
Outputs:
- nearest: float32 [65536], P(('groups', 'blk', 'span')), parts along dimension 0
- centroid_cosine: float32 [65536], P(('groups', 'blk', 'span')), parts along dimension 0
The draws below stay inside these ranges and needn't reach their ends.
There are 4 independent parts, one for each index of `groups`. The reference program is written for one: setup_inputs(seed, part) draws one part's arguments, and reference() takes and returns one part's arrays. A program takes and returns all parts, laid end to end along the dimension named above; each array names one. Nothing has to cross between parts.
Inputs may be any that keep to these rules, and one draw needn't show every extreme that they name: `owner_ids`: at most 16 rows of one device name the same owner; in every draw one owner is named by exactly 16 rows of every device. `local_ids`: of the rows of one device that name one owner, at most 4 have local id 0; in every draw one owner receives exactly 4 rows with local id 0 from every device. In every draw some clusters with a local id other than 0 have exactly one row in the whole shard. cluster_map[o * 16 + l] = o * 16 + l for l > 0. For l = 0 the owners fall into runs of 1 to 3 consecutive owners, and every owner of a run has the value of the run's first owner; some run has 3 owners.
All inputs are finite; a program needn't handle non-finite values.
Results may differ from the reference program's by a relative error of at most 0.0017.
Values may be sent and summed in bfloat16 or wider, within the bound.
A program may use at most 64 MiB of HBM per device.

```python
import jax
import jax.numpy as jnp
from jax import lax

D = 768
ROWS_DEV = 256
OWNED = 16
GIANT_SPAN = 3
ROWS = 16384
CAPACITY = 16
SHARED = 4
CLUSTERS = 512
N_BLK = 32
N_SPAN = 2


def routing(key):
    keys = jax.random.split(key, 9)
    devices = N_BLK * N_SPAN
    candidates = N_BLK * CAPACITY
    owner_range = jnp.arange(N_BLK, dtype=jnp.int32)
    busy = jax.random.randint(keys[0], (), 0, N_BLK)
    slot_owner = jnp.arange(candidates, dtype=jnp.int32) // CAPACITY
    slot_rank = jnp.arange(candidates, dtype=jnp.int32) % CAPACITY
    weights = jax.random.randint(keys[1], (devices, N_BLK), 0, 8192)
    weights = jnp.where(owner_range[None, :] == busy, 1 << 20, weights)
    noise = jax.random.randint(keys[2], (devices, candidates), 0, 4096)
    score = (noise + weights[:, slot_owner]) * candidates + jnp.arange(candidates, dtype=jnp.int32)[None, :]
    chosen = jnp.argsort(-score, axis=1)[:, :ROWS_DEV]
    shuffle = jax.vmap(lambda k: jax.random.permutation(k, ROWS_DEV))(jax.random.split(keys[3], devices))
    chosen = jnp.take_along_axis(chosen, shuffle, axis=1)
    owners = slot_owner[chosen]
    ranks = slot_rank[chosen]
    share_count = jax.random.randint(keys[4], (devices, N_BLK), 0, SHARED + 1)
    share_count = jnp.where(owner_range[None, :] == busy, SHARED, share_count)
    shared = ranks < jnp.take_along_axis(share_count, owners, axis=1)
    lone = jax.random.randint(keys[5], (N_BLK,), 1, OWNED)
    flagged = (jax.random.randint(keys[6], (N_BLK,), 0, 2) == 1) | (owner_range == busy)
    first_pick = jax.random.randint(keys[7], (devices, ROWS_DEV), 0, OWNED - 2)
    second_pick = jax.random.randint(keys[8], (devices, ROWS_DEV), 0, OWNED - 2)
    skewed = jnp.minimum(first_pick, second_pick).reshape(ROWS)
    owner_flat = owners.reshape(ROWS).astype(jnp.int32)
    shared_flat = shared.reshape(ROWS)
    lone_row = lone[owner_flat]
    other = 1 + (lone_row + skewed) % (OWNED - 1)
    row_index = jnp.arange(ROWS, dtype=jnp.int32)
    open_rows = (owner_flat[:, None] == owner_range[None, :]) & jnp.logical_not(shared_flat)[:, None]
    first_row = jnp.min(jnp.where(open_rows, row_index[:, None], ROWS), axis=0)
    single = flagged[owner_flat] & (first_row[owner_flat] == row_index)
    local = jnp.where(shared_flat, 0, jnp.where(single, lone_row, other))
    return (owner_flat.reshape(ROWS, 1).astype(jnp.int32), local.astype(jnp.int32))


def draw_owner_ids(key, part):
    return routing(jax.random.fold_in(key, 11))[0]


def draw_local_ids(key, part):
    return routing(jax.random.fold_in(key, 11))[1]


def draw_cluster_map(key, part):
    first, second = jax.random.split(jax.random.fold_in(key, 7))
    lengths = jax.random.randint(first, (N_BLK,), 1, GIANT_SPAN + 1)
    forced = jax.random.randint(second, (), 0, max(1, N_BLK // GIANT_SPAN - 1))
    owner = jnp.arange(N_BLK, dtype=jnp.int32)
    lengths = jnp.where(owner == forced, GIANT_SPAN, lengths)
    starts = jnp.cumsum(lengths) - lengths
    inside = starts[None, :] <= owner[:, None]
    run_start = jnp.max(jnp.where(inside, starts[None, :], 0), axis=1)
    local = jnp.arange(OWNED, dtype=jnp.int32)
    base = owner[:, None] * OWNED + local[None, :]
    merged = jnp.where(local[None, :] == 0, run_start[:, None] * OWNED, base)
    return merged.reshape(CLUSTERS).astype(jnp.int32)


def level_of(stream_key, shape, pieces, low, high):
    def one(position, blocks):
        draws = jax.random.uniform(jax.random.fold_in(jax.random.fold_in(stream_key, 6), position), (blocks,), jnp.float32, low / len(pieces), high / len(pieces))
        return jnp.repeat(jnp.exp(draws), shape[position] // blocks).reshape((-1,) + (1,) * (len(shape) - position - 1))

    loudness = one(*pieces[0])
    for cut in pieces[1:]:
        loudness = loudness * one(*cut)
    return loudness


def gaussian(key, dims, deviation, bound, shards=(), kind=jnp.bfloat16):
    result = jax.random.normal(key, dims, jnp.float32) * deviation
    if len(shards) > 0:
        result = level_of(key, dims, shards, -0.22, 0.18) * result
    return jnp.clip(result, min=-bound, max=bound).astype(kind)


def setup_inputs(seed: int = 0, part: int = 0) -> dict:
    key_list = jax.random.split(jax.random.key(seed), 5)
    part_splits = jax.random.split(jax.random.fold_in(key_list[4], part), 5)
    embeddings = gaussian(part_splits[0], (ROWS, D), 1.0, 6.0, ((0, 64),))
    owner_ids = draw_owner_ids(jax.random.fold_in(jax.random.fold_in(key_list[4], part), 71), part)
    local_ids = draw_local_ids(jax.random.fold_in(jax.random.fold_in(key_list[4], part), 71), part)
    cluster_map = draw_cluster_map(jax.random.fold_in(jax.random.fold_in(key_list[4], part), 71), part)
    return {"embeddings": embeddings, "owner_ids": owner_ids, "local_ids": local_ids, "cluster_map": cluster_map}


def normalize(values):
    wide = values.astype(jnp.float32)
    scale = lax.rsqrt(lax.optimization_barrier(jnp.sum(wide * wide, axis=1, keepdims=True)) + 1e-06)
    return (wide * scale).astype(jnp.bfloat16)

def reference(embeddings, owner_ids, local_ids, cluster_map):
    unit = normalize(embeddings)
    flat = (owner_ids[:, 0] * OWNED + local_ids).astype(jnp.int32)
    cluster = cluster_map[flat].astype(jnp.int32)
    wide = unit.astype(jnp.float32)
    sums = jax.ops.segment_sum(wide, cluster, num_segments=CLUSTERS)
    length = jnp.sqrt(lax.optimization_barrier(jnp.sum(sums * sums, axis=1, keepdims=True)))
    direction = sums / jnp.maximum(length, 1.0)
    centroid_cosine = lax.optimization_barrier(jnp.sum(wide * direction[cluster], axis=1))
    total = unit.shape[0]
    every = jnp.arange(total, dtype=jnp.int32)

    def one_block(start):
        piece = lax.dynamic_slice_in_dim(unit, start, ROWS_DEV, 0)
        tags = lax.dynamic_slice_in_dim(cluster, start, ROWS_DEV, 0)
        scores = jnp.dot(piece, unit.T, preferred_element_type=jnp.float32)
        index = start + jnp.arange(ROWS_DEV, dtype=jnp.int32)
        keep = (tags[:, None] == cluster[None, :]) & (index[:, None] != every[None, :])
        return lax.optimization_barrier(jnp.max(jnp.where(keep, scores, -1.0), axis=1))
    starts = jnp.arange(total // ROWS_DEV, dtype=jnp.int32) * ROWS_DEV
    nearest = lax.map(one_block, starts).reshape(total)
    return (nearest, centroid_cosine)
```

```python
import functools

import jax
import jax.numpy as jnp
from jax import lax
from jax.experimental import pallas as pl
from jax.experimental.pallas import tpu as pltpu
from jax.sharding import PartitionSpec as P

MESH = pl.DeviceIdType.MESH
LANES = 128
F32 = jnp.float32
BF16 = jnp.bfloat16


def dot(left, right, dims, precision=None):
    return lax.dot_general(
        left, right, (dims, ((), ())), preferred_element_type=F32, precision=precision
    )


def iota(shape, dim):
    return lax.broadcasted_iota(jnp.int32, shape, dim)


def column(row):
    eye = iota((LANES, LANES), 0) == iota((LANES, LANES), 1)
    pieces = []
    for at in range(0, row.shape[1], LANES):
        piece = jnp.where(eye, row[:, at : at + LANES], 0.0)
        pieces.append(jnp.sum(piece, axis=1, keepdims=True))
    return jnp.concatenate(pieces, axis=0)


def farthest_first(j, owners):
    return owners // 2 + (1 - 2 * lax.rem(j, 2)) * ((j + 1) // 2)


def kernel(
    owners,
    capacity,
    shared,
    owned,
    emb_hbm,
    owner_hbm,
    local_hbm,
    map_hbm,
    near_ref,
    cos_ref,
    emb,
    owner_row,
    local_row,
    map_row,
    place,
    packed,
    tags_out,
    mine,
    peer,
    tags_in,
    tags_mine,
    tags_peer,
    giant,
    giant_tags,
    side,
    side_peer,
    side_tags,
    side_tags_peer,
    mid_out,
    mid_in,
    reply_out,
    reply_in,
    in_sem,
    row_send,
    row_recv,
    tag_send,
    tag_recv,
    peer_send,
    peer_recv,
    ptag_send,
    ptag_recv,
    side_send,
    side_recv,
    stag_send,
    stag_recv,
    spx_send,
    spx_recv,
    spt_send,
    spt_recv,
    mid_send,
    mid_recv,
    reply_send,
    reply_recv,
):
    me = lax.axis_index("blk")
    half = lax.axis_index("span")
    rows, width = emb_hbm.shape
    slots = owners * capacity
    per_chunk = LANES // capacity
    chunks = slots // LANES
    many = owners * shared

    def at(step):
        return {"blk": lax.rem(me + step, owners), "span": half}

    other = {"blk": me, "span": 1 - half}

    barrier = pltpu.get_barrier_semaphore()

    def greet(j, carry):
        step = farthest_first(j, owners)
        pl.semaphore_signal(barrier, inc=1, device_id=at(step), device_id_type=MESH)
        return carry

    loads = [
        pltpu.make_async_copy(source, target, in_sem.at[i])
        for i, (source, target) in enumerate(
            (
                (emb_hbm, emb),
                (owner_hbm, owner_row),
                (local_hbm, local_row),
                (map_hbm, map_row),
            )
        )
    ]
    for load in loads:
        load.start()
    lax.fori_loop(0, owners - 1, greet, 0)
    pl.semaphore_signal(barrier, inc=1, device_id=other, device_id_type=MESH)
    for load in loads:
        load.wait()

    relative = owner_row[...] - me
    relative = jnp.where(relative < 0, relative + owners, relative)
    local = local_row[...]
    to_owner = relative == iota((owners, rows), 0)
    first = local == 0
    one_first = jnp.where(to_owner & first, 1.0, 0.0)
    one_rest = jnp.where(to_owner & ~first, 1.0, 0.0)
    before = jnp.where(iota((rows, rows), 0) < iota((rows, rows), 1), 1.0, 0.0).astype(BF16)
    both = jnp.concatenate([one_first, one_rest], axis=0).astype(BF16)
    prefix = dot(both, before, ((1,), (0,)))
    heads = jnp.sum(one_first, axis=1, keepdims=True)
    rank = jnp.sum(
        one_first * prefix[:owners] + one_rest * (prefix[owners:] + heads), axis=0, keepdims=True
    )
    position = relative.astype(F32) * capacity + rank
    placed = jnp.where(iota((slots, rows), 0).astype(F32) == position, 1.0, 0.0).astype(BF16)
    place[...] = placed

    wide = emb[...].astype(F32)
    scale = lax.rsqrt(jnp.sum(wide * wide, axis=1, keepdims=True) + 1e-06)
    unit = (wide * scale).astype(BF16)
    packed[...] = (
        dot(placed, unit, ((1,), (0,))).astype(BF16).reshape(owners, capacity, width)
    )
    tag_lhs = jnp.broadcast_to((local + 1).astype(F32), (8, rows)).astype(BF16)
    tag_row = dot(tag_lhs, placed, ((1,), (1,)))[:1]
    for c in range(chunks):
        tags_out[c] = tag_row[:, c * LANES : (c + 1) * LANES]
    mine[0] = packed[0]
    tags_in[0] = tags_out[0]

    pl.semaphore_wait(barrier, owners)

    def send_rows(step):
        return pltpu.make_async_remote_copy(
            src_ref=packed.at[step],
            dst_ref=mine.at[step],
            send_sem=row_send.at[step],
            recv_sem=row_recv.at[step],
            device_id=at(step),
            device_id_type=MESH,
        )

    def send_tags(step):
        return pltpu.make_async_remote_copy(
            src_ref=tags_out.at[step // per_chunk],
            dst_ref=tags_in.at[step],
            send_sem=tag_send.at[step],
            recv_sem=tag_recv.at[step],
            device_id=at(step),
            device_id_type=MESH,
        )

    def to_peer(source, step):
        return pltpu.make_async_remote_copy(
            src_ref=source.at[step],
            dst_ref=peer.at[step],
            send_sem=peer_send.at[step],
            recv_sem=peer_recv.at[step],
            device_id=other,
            device_id_type=MESH,
        )

    def start_rows(j, carry):
        step = farthest_first(j, owners)
        send_tags(step).start()
        send_rows(step).start()
        return carry

    lax.fori_loop(0, owners - 1, start_rows, 0)
    to_peer(packed, 0).start()

    def take_rows(j, carry):
        step = farthest_first(j, owners)
        send_tags(step).wait_recv()
        send_rows(step).wait_recv()
        to_peer(mine, step).start()
        return carry

    lax.fori_loop(0, owners - 1, take_rows, 0)

    lane_group = iota((1, LANES), 1) // capacity
    row_parts = []
    for c in range(chunks):
        part = jnp.zeros((1, LANES), F32)
        for g in range(per_chunk):
            part = jnp.where(lane_group == g, tags_in[c * per_chunk + g], part)
        tags_mine[c] = part
        row_parts.append(part)
    my_tags = jnp.concatenate(row_parts, axis=1)
    peer_tags_copy = pltpu.make_async_remote_copy(
        src_ref=tags_mine,
        dst_ref=tags_peer,
        send_sem=ptag_send,
        recv_sem=ptag_recv,
        device_id=other,
        device_id_type=MESH,
    )
    peer_tags_copy.start()

    own_rows = mine[...].reshape(slots, width)
    slot_of = capacity * (iota((many, slots), 0) // shared) + lax.rem(
        iota((many, slots), 0), shared
    )
    picked = slot_of == iota((many, slots), 1)
    giant[...] = dot(jnp.where(picked, 1.0, 0.0).astype(BF16), own_rows, ((1,), (0,))).astype(
        BF16
    )
    my_column = column(my_tags)
    slot_back = capacity * (iota((slots, many), 1) // shared) + lax.rem(
        iota((slots, many), 1), shared
    )
    picked_back = slot_back == iota((slots, many), 0)
    giant_tags[0] = jnp.sum(
        jnp.where(picked_back & (my_column == 1.0), 1.0, 0.0), axis=0, keepdims=True
    )

    def to_side(which):
        step = 1 if which == 0 else owners - 1
        return (
            pltpu.make_async_remote_copy(
                src_ref=giant,
                dst_ref=side.at[which],
                send_sem=side_send.at[which],
                recv_sem=side_recv.at[which],
                device_id=at(step),
                device_id_type=MESH,
            ),
            pltpu.make_async_remote_copy(
                src_ref=giant_tags.at[0],
                dst_ref=side_tags.at[which],
                send_sem=stag_send.at[which],
                recv_sem=stag_recv.at[which],
                device_id=at(step),
                device_id_type=MESH,
            ),
        )

    sides = [to_side(0), to_side(1)]
    for copies in sides:
        for copy in copies:
            copy.start()

    best = jnp.full((1, slots), -1.0, F32)
    block = 256
    for at_row in range(0, slots, block):
        part = own_rows[at_row : at_row + block]
        scores = dot(part, own_rows, ((1,), (1,)))
        same = my_column[at_row : at_row + block] == my_tags
        itself = (iota((block, slots), 0) + at_row) == iota((block, slots), 1)
        scores = jnp.where(same & ~itself, scores, -1.0)
        best = jnp.maximum(best, jnp.max(scores, axis=0, keepdims=True))

    peer_tags_copy.wait_recv()
    for step in range(owners):
        to_peer(packed if step == 0 else mine, step).wait_recv()
    peer_row = jnp.concatenate([tags_peer[c] for c in range(chunks)], axis=1)
    peer_column = column(peer_row)
    peer_rows = peer[...].reshape(slots, width)
    for at_row in range(0, slots, block):
        part = peer_rows[at_row : at_row + block]
        scores = dot(part, own_rows, ((1,), (1,)))
        same = peer_column[at_row : at_row + block] == my_tags
        scores = jnp.where(same, scores, -1.0)
        best = jnp.maximum(best, jnp.max(scores, axis=0, keepdims=True))
    ids = (iota((owned, slots), 0) + 1).astype(F32)
    sums = dot(jnp.where(ids == my_tags, 1.0, 0.0).astype(BF16), own_rows, ((1,), (0,)))
    sums += dot(jnp.where(ids == peer_row, 1.0, 0.0).astype(BF16), peer_rows, ((1,), (0,)))

    def side_to_peer(which):
        return (
            pltpu.make_async_remote_copy(
                src_ref=side.at[which],
                dst_ref=side_peer.at[which],
                send_sem=spx_send.at[which],
                recv_sem=spx_recv.at[which],
                device_id=other,
                device_id_type=MESH,
            ),
            pltpu.make_async_remote_copy(
                src_ref=side_tags.at[which],
                dst_ref=side_tags_peer.at[which],
                send_sem=spt_send.at[which],
                recv_sem=spt_recv.at[which],
                device_id=other,
                device_id_type=MESH,
            ),
        )

    shares = [side_to_peer(0), side_to_peer(1)]
    for copies, share in zip(sides, shares):
        for copy, on in zip(copies, share):
            copy.wait_recv()
            on.start()
    for share in shares:
        for on in share:
            on.wait_recv()

    lane = iota(map_row.shape, 1)

    def number(step):
        owner = lax.rem(me + step, owners)
        return jnp.sum(
            jnp.where(lane == owner * owned, map_row[...], 0), axis=1, keepdims=True
        )

    here, up, down = number(0), number(1), number(owners - 1)
    near = [jnp.where(here == down, 1.0, 0.0), jnp.where(here == up, 1.0, 0.0)]
    across = jnp.where(up == down, 1.0, 0.0)

    rows_of = [jnp.concatenate([side[w], side_peer[w]], axis=0) for w in (0, 1)]
    tags_of = [jnp.concatenate([side_tags[w], side_tags_peer[w]], axis=1) for w in (0, 1)]
    columns_of = [column(t) for t in tags_of]
    side_sums = [
        dot(jnp.broadcast_to(tags_of[w], (8, 2 * many)).astype(BF16), rows_of[w], ((1,), (0,)))[:1]
        for w in (0, 1)
    ]
    for w in (0, 1):
        far = 1 - w
        scores = dot(rows_of[far], side[w], ((1,), (1,)))
        keep = (columns_of[far] * across) > 0.5
        top = jnp.max(jnp.where(keep, scores, -1.0), axis=0, keepdims=True)
        mid_out[w, :, :LANES] = top
        mid_out[w, :, LANES:] = side_sums[far] * across

    def to_mid(w):
        return pltpu.make_async_remote_copy(
            src_ref=mid_out.at[w],
            dst_ref=mid_in.at[1 - w],
            send_sem=mid_send.at[w],
            recv_sem=mid_recv.at[1 - w],
            device_id=at(owners - 1 if w == 0 else 1),
            device_id_type=MESH,
        )

    def from_mid(w):
        return pltpu.make_async_remote_copy(
            src_ref=mid_out.at[w],
            dst_ref=mid_in.at[w],
            send_sem=mid_send.at[w],
            recv_sem=mid_recv.at[w],
            device_id=at(owners - 1 if w == 0 else 1),
            device_id_type=MESH,
        )

    for w in (0, 1):
        to_mid(w).start()

    shared_here = my_tags == 1.0
    for w in (0, 1):
        scores = dot(rows_of[w], own_rows, ((1,), (1,)))
        keep = ((columns_of[w] * near[w]) > 0.5) & shared_here
        best = jnp.maximum(
            best, jnp.max(jnp.where(keep, scores, -1.0), axis=0, keepdims=True)
        )
    extra = side_sums[0] * near[0] + side_sums[1] * near[1]

    for w in (0, 1):
        from_mid(w).wait_recv()
    top = jnp.maximum(mid_in[0, :, :LANES], mid_in[1, :, :LANES])
    spread = jnp.max(jnp.where(picked, column(top), -1.0), axis=0, keepdims=True)
    best = jnp.maximum(best, jnp.where(shared_here, spread, -1.0))
    extra += mid_in[0, :, LANES:] + mid_in[1, :, LANES:]
    sums += jnp.where(iota((owned, width), 0) == 0, extra, 0.0)

    length = jnp.sqrt(jnp.sum(sums * sums, axis=1, keepdims=True))
    direction = sums / jnp.maximum(length, 1.0)
    high = direction.astype(BF16)
    low = (direction - high.astype(F32)).astype(BF16)
    cosines = dot(jnp.concatenate([high, low], axis=0), own_rows, ((1,), (1,)))
    cosines = cosines[:owned] + cosines[owned:]
    cosine = jnp.sum(jnp.where(ids == my_tags, cosines, 0.0), axis=0, keepdims=True)

    for c in range(chunks):
        reply_out[c, 0:1] = best[:, c * LANES : (c + 1) * LANES]
        reply_out[c, 1:2] = cosine[:, c * LANES : (c + 1) * LANES]

    def send_reply(step):
        return pltpu.make_async_remote_copy(
            src_ref=reply_out.at[step // per_chunk],
            dst_ref=reply_in.at[step],
            send_sem=reply_send.at[step],
            recv_sem=reply_recv.at[step],
            device_id=at(owners - step),
            device_id_type=MESH,
        )

    def start_reply(j, carry):
        send_reply(farthest_first(j, owners)).start()
        return carry

    lax.fori_loop(0, owners - 1, start_reply, 0)
    reply_in[0] = reply_out[0]

    def drain(j, carry):
        step = farthest_first(j, owners)
        send_rows(step).wait_send()
        send_tags(step).wait_send()
        to_peer(mine, step).wait_send()
        return carry

    lax.fori_loop(0, owners - 1, drain, 0)
    to_peer(packed, 0).wait_send()
    peer_tags_copy.wait_send()
    for copies in sides + shares:
        for copy in copies:
            copy.wait_send()
    for w in (0, 1):
        to_mid(w).wait_send()

    def take_reply(j, carry):
        step = owners - 1 - j
        send_reply(step).wait()
        return carry

    lax.fori_loop(0, owners - 1, take_reply, 0)

    parts = []
    for c in range(chunks):
        part = jnp.zeros((2, LANES), F32)
        for g in range(per_chunk):
            part = jnp.where(lane_group == g, reply_in[c * per_chunk + g], part)
        parts.append(part)
    values = jnp.concatenate(parts, axis=1)
    one = values.astype(BF16)
    rest = values - one.astype(F32)
    two = rest.astype(BF16)
    three = (rest - two.astype(F32)).astype(BF16)
    chosen = dot(jnp.concatenate([one, two, three], axis=0), place[...], ((1,), (0,)))
    result = chosen[0:2] + chosen[2:4] + chosen[4:6]
    near_ref[...] = result[0:1]
    cos_ref[...] = result[1:2]


def body(embeddings, owner_ids, local_ids, cluster_map):
    rows, width = embeddings.shape
    owners = lax.axis_size("blk")
    capacity = 2 * rows // owners
    shared = max(1, capacity // 4)
    slots = owners * capacity
    clusters = cluster_map.shape[0]
    owned = clusters // owners
    chunks = slots // LANES
    many = owners * shared
    dma = pltpu.SemaphoreType.DMA
    vmem = pltpu.VMEM
    near, cosine = pl.pallas_call(
        functools.partial(kernel, owners, capacity, shared, owned),
        out_shape=[jax.ShapeDtypeStruct((1, rows), F32)] * 2,
        in_specs=[pl.BlockSpec(memory_space=pl.ANY)] * 4,
        out_specs=[pl.BlockSpec(memory_space=pltpu.VMEM)] * 2,
        scratch_shapes=[
            vmem((rows, width), BF16),
            vmem((1, rows), jnp.int32),
            vmem((1, rows), jnp.int32),
            vmem((1, clusters), jnp.int32),
            vmem((slots, rows), BF16),
            vmem((owners, capacity, width), BF16),
            vmem((chunks, 1, LANES), F32),
            vmem((owners, capacity, width), BF16),
            vmem((owners, capacity, width), BF16),
            vmem((owners, 1, LANES), F32),
            vmem((chunks, 1, LANES), F32),
            vmem((chunks, 1, LANES), F32),
            vmem((many, width), BF16),
            vmem((1, 1, LANES), F32),
            vmem((2, many, width), BF16),
            vmem((2, many, width), BF16),
            vmem((2, 1, LANES), F32),
            vmem((2, 1, LANES), F32),
            vmem((2, 1, LANES + width), F32),
            vmem((2, 1, LANES + width), F32),
            vmem((chunks, 2, LANES), F32),
            vmem((owners, 2, LANES), F32),
            dma((4,)),
            dma((owners,)),
            dma((owners,)),
            dma((owners,)),
            dma((owners,)),
            dma((owners,)),
            dma((owners,)),
            dma,
            dma,
            dma((2,)),
            dma((2,)),
            dma((2,)),
            dma((2,)),
            dma((2,)),
            dma((2,)),
            dma((2,)),
            dma((2,)),
            dma((2,)),
            dma((2,)),
            dma((owners,)),
            dma((owners,)),
        ],
        compiler_params=pltpu.CompilerParams(collective_id=0, has_side_effects=True),
    )(
        embeddings,
        owner_ids.reshape(1, rows),
        local_ids.reshape(1, rows),
        cluster_map.reshape(1, clusters),
    )
    return near.reshape(rows), cosine.reshape(rows)


def solution(mesh):
    return jax.shard_map(
        body,
        mesh=mesh,
        in_specs=(
            P(("groups", "blk", "span"), None),
            P(("groups", "blk", "span"), None),
            P(("groups", "blk", "span")),
            P("groups"),
        ),
        out_specs=(P(("groups", "blk", "span")), P(("groups", "blk", "span"))),
        check_vma=False,
    )
```
